16 devices in a mesh: dp: 4 (over z, y), ep: 4 (over x, core).
Axes of the slice: x: 2, y: 2, z: 2, core: 2. Of those that a mesh axis runs over, the one named last changes fastest.
Arguments:
- hidden_in: bfloat16 [4096, 2560], P(('dp', 'ep')), parts along dimension 0
- topk_idx: int32 [4096, 6], P(('dp', 'ep')), parts along dimension 0
- norm_gain: bfloat16 [2560], replicated
- w_router: bfloat16 [2560, 64], replicated
- w_sgate: bfloat16 [2560, 1], replicated
- s_gate: bfloat16 [2560, 3072], replicated
- s_up: bfloat16 [2560, 3072], replicated
- s_down: bfloat16 [3072, 2560], replicated
- w_gate: bfloat16 [64, 2560, 1536], P('ep')
- w_up: bfloat16 [64, 2560, 1536], P('ep')
- w_down: bfloat16 [64, 1536, 2560], P('ep')
Outputs:
- output: bfloat16 [4096, 2560], P(('dp', 'ep')), parts along dimension 0
There are 4 independent parts. The reference program is written for one: setup_inputs(seed, part) draws one part's arguments, and reference() takes and returns one part's arrays. A program takes and returns all parts, laid end to end along the dimension named above; an argument that names none is the same for every part.
All inputs are finite; a program needn't handle non-finite values.
Results may differ from the reference program's by a relative error of at most 0.001.
Values are sent between devices in bfloat16 or wider.
A program may use at most 1.75 GiB of HBM per device.

```python
import jax
import jax.numpy as jnp
from jax import lax

HIDDEN = 2560
EXPERTS = 64
EXPERT_SLOTS = 64
TOP_K = 6
EXPERT_FF = 1536
SHARED_FF = 3072
TOKENS_DEV = 256
GROUP_SIZE = 4

TOKENS = TOKENS_DEV * GROUP_SIZE
CAPACITY = (5 * TOKENS * TOP_K + 4 * EXPERTS - 1) // (4 * EXPERTS)
LOCAL_MAX = (2 * TOKENS_DEV * TOP_K + EXPERTS - 1) // EXPERTS
HOT_COUNT = EXPERTS // 4


def row_order(sub_key):
    return jax.random.permutation(sub_key, TOKENS_DEV)


def draw_routing(route_key):
    key_perm, key_shift, key_rows, key_cols = jax.random.split(route_key, 4)
    per_dev = TOKENS_DEV * TOP_K
    base_perm = jax.random.permutation(key_perm, EXPERTS)
    shifts = jax.random.randint(key_shift, (GROUP_SIZE,), 0, HOT_COUNT)
    pos_index = jnp.arange(per_dev)
    hot_total = HOT_COUNT * LOCAL_MAX
    rest_total = per_dev - hot_total
    rank_seq = jnp.where(pos_index < hot_total, pos_index // LOCAL_MAX,
                         HOT_COUNT + ((pos_index - hot_total) * (EXPERTS - HOT_COUNT)) // rest_total)
    choice = base_perm[(rank_seq[None, :] + shifts[:, None]) % EXPERTS]
    choice = choice.reshape(GROUP_SIZE, TOP_K, TOKENS_DEV).transpose(0, 2, 1)
    row_perm = jax.vmap(row_order)(jax.random.split(key_rows, GROUP_SIZE))
    choice = jnp.take_along_axis(choice, row_perm[:, :, None], axis=1)
    scores = jax.random.randint(key_cols, (GROUP_SIZE, TOKENS_DEV, TOP_K), 0, 1 << 20) * TOP_K + jnp.arange(TOP_K)
    choice = jnp.take_along_axis(choice, jnp.argsort(scores, axis=2), axis=2)
    return choice.reshape(TOKENS, TOP_K).astype(jnp.int32)


def setup_inputs(seed: int = 0, part: int = 0) -> dict:
    base_key = jax.random.key(seed)
    key_x, key_route = jax.random.split(jax.random.fold_in(base_key, part))
    weight_keys = jax.random.split(base_key, 9)
    in_scale = HIDDEN ** -0.5
    down_scale = (EXPERTS / TOP_K) * EXPERT_FF ** -0.5
    live_mask = (jnp.arange(EXPERT_SLOTS) < EXPERTS).astype(jnp.float32)[:, None, None]
    return {
        'hidden_in': (0.5 * jax.random.normal(key_x, (TOKENS, HIDDEN), jnp.float32)).astype(jnp.bfloat16),
        'topk_idx': draw_routing(key_route),
        'norm_gain': (1.0 + 0.3 * jax.random.normal(weight_keys[0], (HIDDEN,), jnp.float32)).astype(jnp.bfloat16),
        'w_router': (in_scale * jax.random.normal(weight_keys[1], (HIDDEN, EXPERTS), jnp.float32)).astype(jnp.bfloat16),
        'w_sgate': (in_scale * jax.random.normal(weight_keys[2], (HIDDEN, 1), jnp.float32)).astype(jnp.bfloat16),
        's_gate': (in_scale * jax.random.normal(weight_keys[3], (HIDDEN, SHARED_FF), jnp.float32)).astype(jnp.bfloat16),
        's_up': (in_scale * jax.random.normal(weight_keys[4], (HIDDEN, SHARED_FF), jnp.float32)).astype(jnp.bfloat16),
        's_down': (SHARED_FF ** -0.5 * jax.random.normal(weight_keys[5], (SHARED_FF, HIDDEN), jnp.float32)).astype(jnp.bfloat16),
        'w_gate': (in_scale * live_mask * jax.random.normal(weight_keys[6], (EXPERT_SLOTS, HIDDEN, EXPERT_FF), jnp.float32)).astype(jnp.bfloat16),
        'w_up': (in_scale * live_mask * jax.random.normal(weight_keys[7], (EXPERT_SLOTS, HIDDEN, EXPERT_FF), jnp.float32)).astype(jnp.bfloat16),
        'w_down': (down_scale * live_mask * jax.random.normal(weight_keys[8], (EXPERT_SLOTS, EXPERT_FF, HIDDEN), jnp.float32)).astype(jnp.bfloat16),
    }


def rms_norm(hidden_in, norm_gain):
    x_f32 = hidden_in.astype(jnp.float32)
    inv_rms = lax.rsqrt(jnp.mean(x_f32 * x_f32, axis=-1, keepdims=True) + 1e-6)
    return (x_f32 * inv_rms * norm_gain.astype(jnp.float32)).astype(jnp.bfloat16)


def expert_mlp(operands):
    expert_rows, gate_w, up_w, down_w = operands
    expert_act = (jax.nn.silu(jnp.dot(expert_rows, gate_w, preferred_element_type=jnp.float32))
                  * jnp.dot(expert_rows, up_w, preferred_element_type=jnp.float32)).astype(jnp.bfloat16)
    return jnp.dot(expert_act, down_w, preferred_element_type=jnp.float32).astype(jnp.bfloat16)


def reference(hidden_in, topk_idx, norm_gain, w_router, w_sgate, s_gate, s_up, s_down, w_gate, w_up, w_down):
    normed = rms_norm(hidden_in, norm_gain)
    router_probs = jax.nn.softmax(jnp.dot(normed, w_router, preferred_element_type=jnp.float32), axis=-1)
    gate_vals = jnp.take_along_axis(router_probs, topk_idx, axis=1)
    flat_ids = topk_idx.reshape(-1)
    onehot = (flat_ids[:, None] == jnp.arange(EXPERTS)[None, :]).astype(jnp.int32)
    position = jnp.sum((jnp.cumsum(onehot, axis=0) - onehot) * onehot, axis=1)
    slot_pos = jnp.where(position < CAPACITY, flat_ids * CAPACITY + position, EXPERTS * CAPACITY)
    token_of = jnp.arange(TOKENS * TOP_K) // TOP_K
    row_table = jnp.full((EXPERTS * CAPACITY,), TOKENS, jnp.int32).at[slot_pos].set(token_of, mode='drop')
    expert_rows = jnp.take(normed, row_table, axis=0, mode='fill', fill_value=0).reshape(EXPERTS, CAPACITY, HIDDEN)
    results = lax.map(expert_mlp, (expert_rows, w_gate[:EXPERTS], w_up[:EXPERTS], w_down[:EXPERTS]))
    picked = jnp.take(results.reshape(EXPERTS * CAPACITY, HIDDEN), slot_pos, axis=0, mode='fill', fill_value=0)
    picked = picked.reshape(TOKENS, TOP_K, HIDDEN)
    routed = jnp.sum(gate_vals[:, :, None] * picked.astype(jnp.float32), axis=1)
    shared_act = (jax.nn.silu(jnp.dot(normed, s_gate, preferred_element_type=jnp.float32))
                  * jnp.dot(normed, s_up, preferred_element_type=jnp.float32)).astype(jnp.bfloat16)
    shared_val = jnp.dot(shared_act, s_down, preferred_element_type=jnp.float32)
    shared_gate = jax.nn.sigmoid(jnp.dot(normed, w_sgate, preferred_element_type=jnp.float32))
    return (hidden_in.astype(jnp.float32) + routed + shared_gate * shared_val).astype(jnp.bfloat16)
```

```python
import functools

import jax
import jax.numpy as jnp
from jax import lax
from jax.experimental import pallas as pl
from jax.experimental.pallas import tpu as pltpu
from jax.sharding import PartitionSpec as P

F32 = jnp.float32
BF16 = jnp.bfloat16
LANES = 128


def rms_norm(hidden_in, norm_gain):
    x_f32 = hidden_in.astype(F32)
    inv_rms = lax.rsqrt(jnp.mean(x_f32 * x_f32, axis=-1, keepdims=True) + 1e-6)
    return (x_f32 * inv_rms * norm_gain.astype(F32)).astype(BF16)


def shared_expert(normed, w_sgate, s_gate, s_up, s_down):
    shared_act = (jax.nn.silu(jnp.dot(normed, s_gate, preferred_element_type=F32))
                  * jnp.dot(normed, s_up, preferred_element_type=F32)).astype(BF16)
    shared_val = jnp.dot(shared_act, s_down, preferred_element_type=F32)
    return jax.nn.sigmoid(jnp.dot(normed, w_sgate, preferred_element_type=F32)) * shared_val


def kept_positions(idx, lower, capacity):
    tok = idx.shape[0]
    lane = lax.broadcasted_iota(jnp.int32, (tok, LANES), 1)
    hit = lane == idx[:, 0:1]
    for k in range(1, idx.shape[1]):
        hit = jnp.logical_or(hit, lane == idx[:, k:k + 1])
    chosen = jnp.where(hit, 1.0, 0.0).astype(F32)
    row = lax.broadcasted_iota(jnp.int32, (tok, tok), 0)
    col = lax.broadcasted_iota(jnp.int32, (tok, tok), 1)
    below = jnp.where(col < row, 1.0, 0.0).astype(BF16)
    pos = jnp.dot(below, chosen.astype(BF16), preferred_element_type=F32)
    kept = jnp.logical_and(hit, pos + lower < capacity)
    return jnp.where(kept, pos, -1.0), lower + jnp.sum(chosen, axis=0, keepdims=True)


def gate_up_kernel(group, slots, local_max, capacity, h_ref, idx_ref, wg_ref, wu_ref, act_ref, pos_ref, x_ref, post_ref, pick_ref):
    expert, part = pl.program_id(0), pl.program_id(1)
    tok = idx_ref.shape[0] // group
    hidden = h_ref.shape[1]
    me = lax.axis_index('ep')

    @pl.when(jnp.logical_and(expert == 0, part == 0))
    def _():
        lower = jnp.zeros((1, LANES), F32)
        for src in range(group):
            pos, lower = kept_positions(idx_ref[src * tok:(src + 1) * tok, :], lower, capacity)
            pos_ref[src * tok:(src + 1) * tok, :] = pos
            post_ref[...] = jnp.transpose(pos)
            n_iota = lax.broadcasted_iota(jnp.int32, (local_max, tok), 0).astype(F32)
            for slot in range(slots):
                row = post_ref[pl.ds(me * slots + slot, 1), :]
                pick_ref[slot * local_max:(slot + 1) * local_max, :] = jnp.where(n_iota == row, 1.0, 0.0).astype(BF16)

            @pl.loop(0, hidden // 256)
            def _(c):
                cols = pl.ds(pl.multiple_of(c * 256, 256), 256)
                rows = jnp.dot(pick_ref[...], h_ref[src * tok:(src + 1) * tok, cols], preferred_element_type=F32)
                x_ref[:, src * local_max:(src + 1) * local_max, cols] = rows.astype(BF16).reshape(slots, local_max, 256)

    rows = x_ref[expert]
    gate = jnp.dot(rows, wg_ref[0], preferred_element_type=F32)
    up = jnp.dot(rows, wu_ref[0], preferred_element_type=F32)
    act_ref[0] = (jax.nn.silu(gate) * up).astype(BF16)


def gate_up(h_all, idx_all, w_gate, w_up, group, capacity, local_max, block=512):
    slots, hidden, ff = w_gate.shape
    tokens = h_all.shape[0]
    tok = tokens // group
    rows = group * local_max
    whole = lambda shape: pl.BlockSpec(shape, lambda e, j: (0,) * len(shape), pipeline_mode=pl.Buffered(1))
    w_spec = pl.BlockSpec((1, hidden, block), lambda e, j: (e, 0, j))
    return pl.pallas_call(
        functools.partial(gate_up_kernel, group, slots, local_max, capacity),
        out_shape=(jax.ShapeDtypeStruct((slots, rows, ff), BF16), jax.ShapeDtypeStruct((tokens, LANES), F32)),
        grid=(slots, ff // block),
        in_specs=[whole((tokens, hidden)), whole(idx_all.shape), w_spec, w_spec],
        out_specs=(pl.BlockSpec((1, rows, block), lambda e, j: (e, 0, j)), pl.BlockSpec((tokens, LANES), lambda e, j: (0, 0))),
        scratch_shapes=[pltpu.VMEM((slots, rows, hidden), BF16), pltpu.VMEM((LANES, tok), F32), pltpu.VMEM((slots * local_max, tok), BF16)],
        compiler_params=pltpu.CompilerParams(vmem_limit_bytes=60 << 20, dimension_semantics=("arbitrary", "arbitrary")),
        cost_estimate=pl.CostEstimate(flops=4 * slots * rows * hidden * ff, bytes_accessed=4 * slots * hidden * ff, transcendentals=0),
        name="gate_up",
    )(h_all, idx_all, w_gate, w_up)


def split3(value):
    high = value.astype(BF16)
    rest = value - high.astype(F32)
    mid = rest.astype(BF16)
    return high, mid, (rest - mid.astype(F32)).astype(BF16)


def combine_weights(pos, prob, me, slots, local_max):
    width = slots * local_max
    slot_of = lax.shift_right_logical(lax.broadcasted_iota(jnp.int32, (LANES, width), 1) * (65536 // local_max + 1), 16)
    spread = jnp.where(lax.broadcasted_iota(jnp.int32, (LANES, width), 0) == slot_of + me * slots, 1.0, 0.0).astype(BF16)
    col = lax.broadcasted_iota(jnp.int32, (pos.shape[0], width), 1)
    place = (col - lax.shift_right_logical(col * (65536 // local_max + 1), 16) * local_max).astype(F32)
    here = jnp.dot(pos.astype(BF16), spread, preferred_element_type=F32) == place
    return [jnp.where(here, jnp.dot(piece, spread, preferred_element_type=F32), 0.0).astype(BF16) for piece in split3(prob)]


def down_kernel(group, slots, local_max, per, act_ref, pos_ref, prob_ref, wd_ref, y_ref, comb_ref, out_ref):
    chunk, step = pl.program_id(0), pl.program_id(1)
    tok = pos_ref.shape[0] // group
    me = lax.axis_index('ep')

    @pl.when(jnp.logical_and(chunk == 0, step == 0))
    def _():
        for dst in range(group):
            rows = slice(dst * tok, (dst + 1) * tok)
            for i, piece in enumerate(combine_weights(pos_ref[rows, :], prob_ref[rows, :], me, slots, local_max)):
                comb_ref[dst, i * tok:(i + 1) * tok, :] = piece

    for i in range(per):
        res = jnp.dot(act_ref[step * per + i], wd_ref[i], preferred_element_type=F32).astype(BF16)
        at = pl.ds(pl.multiple_of((step * per + i) * local_max, local_max), local_max)
        for dst in range(group):
            out_ref[dst, at, :] = res[dst * local_max:(dst + 1) * local_max, :]

    @pl.when(step == pl.num_programs(1) - 1)
    def _():
        for dst in range(group):
            part = jnp.dot(comb_ref[dst], out_ref[dst], preferred_element_type=F32)
            y_ref[dst] = part[:tok] + part[tok:2 * tok] + part[2 * tok:]


def down(act, pos_all, prob_all, w_down, group, local_max, block=512, per=4):
    slots, ff, hidden = w_down.shape
    rows = act.shape[1]
    tokens = pos_all.shape[0]
    tok = tokens // group
    whole = lambda shape: pl.BlockSpec(shape, lambda j, e: (0,) * len(shape), pipeline_mode=pl.Buffered(1))
    return pl.pallas_call(
        functools.partial(down_kernel, group, slots, local_max, per),
        out_shape=jax.ShapeDtypeStruct((group, tok, hidden), F32),
        grid=(hidden // block, slots // per),
        in_specs=[whole(act.shape), whole(pos_all.shape), whole(prob_all.shape),
                  pl.BlockSpec((per, ff, block), lambda j, e: (e, 0, j))],
        out_specs=pl.BlockSpec((group, tok, block), lambda j, e: (0, 0, j)),
        scratch_shapes=[pltpu.VMEM((group, 3 * tok, slots * local_max), BF16), pltpu.VMEM((group, slots * local_max, block), BF16)],
        compiler_params=pltpu.CompilerParams(vmem_limit_bytes=60 << 20, dimension_semantics=("arbitrary", "arbitrary")),
        cost_estimate=pl.CostEstimate(flops=4 * slots * rows * hidden * ff // 2, bytes_accessed=2 * slots * hidden * ff, transcendentals=0),
        name="down",
    )(act, pos_all, prob_all, w_down)


def solution(mesh):
    group = mesh.shape['ep']

    def device_block(hidden_in, topk_idx, norm_gain, w_router, w_sgate, s_gate, s_up, s_down, w_gate, w_up, w_down):
        tok_dev, hidden = hidden_in.shape
        top_k = topk_idx.shape[1]
        experts = w_router.shape[1]
        capacity = (5 * tok_dev * group * top_k + 4 * experts - 1) // (4 * experts)
        local_max = (2 * tok_dev * top_k + experts - 1) // experts
        normed = rms_norm(hidden_in, norm_gain)
        probs = jax.nn.softmax(jnp.dot(normed, w_router, preferred_element_type=F32), axis=-1)
        probs = jnp.pad(probs, ((0, 0), (0, LANES - experts)))
        h_all = lax.all_gather(normed, 'ep', tiled=True)
        idx_all = lax.all_gather(topk_idx, 'ep', tiled=True)
        prob_all = lax.all_gather(probs, 'ep', tiled=True)
        shared_val = shared_expert(normed, w_sgate, s_gate, s_up, s_down)
        act, pos_all = gate_up(h_all, idx_all, w_gate, w_up, group, capacity, local_max)
        parts = down(act, pos_all, prob_all, w_down, group, local_max)
        routed = lax.psum_scatter(parts.reshape(group * tok_dev, hidden), 'ep', tiled=True)
        return (hidden_in.astype(F32) + routed + shared_val).astype(BF16)

    row_spec = P(('dp', 'ep'), None)
    full_spec = P(None, None)
    slot_spec = P('ep', None, None)
    in_specs = (row_spec, row_spec, P(None), full_spec, full_spec, full_spec, full_spec, full_spec,
                slot_spec, slot_spec, slot_spec)
    return jax.shard_map(device_block, mesh=mesh, in_specs=in_specs, out_specs=row_spec, check_vma=False)
```

```python
import functools

import jax
import jax.numpy as jnp
from jax import lax
from jax.experimental import pallas as pl
from jax.experimental.pallas import tpu as pltpu
from jax.sharding import PartitionSpec as P

F32 = jnp.float32
BF16 = jnp.bfloat16
MESH = pl.DeviceIdType.MESH
DEPTH = 4
WIDTH = 512
PIECES = 4


def aligned(start, size):
    return pl.ds(pl.multiple_of(start, size), size)


def moe_kernel(group, experts, capacity, local_max,
               x_hbm, idx_ref, gain_ref, wr_hbm, wsg_ref, sg_hbm, su_hbm, sd_hbm, wg_hbm, wu_hbm, wd_hbm,
               out_hbm,
               ring, xbuf, act, hbuf, pair, relay, fromsib, fromchip, acc, prob, post, sgate, idx_all, wr, counts,
               ring_sem, in_sem, out_sem, idx_send, idx_recv, h_send, h_recv, sib_send, sib_recv, fwd_send, fwd_recv,
               p_send, p_recv, pair_send, pair_recv, relay_send, relay_recv, credit):
    tok, hidden = x_hbm.shape
    slots, _, ff = wg_hbm.shape
    top_k = idx_ref.shape[0]
    rows = group * local_max
    width = slots * local_max
    n_s1 = 2 * ff // WIDTH
    n_s2 = hidden // WIDTH
    parts = ff // WIDTH
    n_g = slots * parts
    n_chunk = hidden // WIDTH
    n_pair = slots // 2
    n_d = n_chunk * n_pair
    first_g, first_d = n_s1 + n_s2, n_s1 + n_s2 + n_g
    total = first_d + n_d
    piece = tok // PIECES

    me = lax.axis_index('ep')
    sib = me + 1 - 2 * lax.rem(me, 2)
    far = lax.rem(me + 2, group)
    diag = lax.rem(sib + 2, group)

    def shared_up(n, s):
        cols = aligned(n * WIDTH, WIDTH)
        return (pltpu.make_async_copy(sg_hbm.at[:, cols], ring.at[s, 0], ring_sem.at[s, 0]),
                pltpu.make_async_copy(su_hbm.at[:, cols], ring.at[s, 1], ring_sem.at[s, 1]))

    def shared_down(n, s):
        cols = aligned(n * WIDTH, WIDTH)
        return tuple(pltpu.make_async_copy(sd_hbm.at[i * ff:(i + 1) * ff, cols], ring.at[s, i, 0:ff, :], ring_sem.at[s, i])
                     for i in range(2))

    def expert_up(n, s):
        e, cols = n // parts, aligned(lax.rem(n, parts) * WIDTH, WIDTH)
        return (pltpu.make_async_copy(wg_hbm.at[e, :, cols], ring.at[s, 0], ring_sem.at[s, 0]),
                pltpu.make_async_copy(wu_hbm.at[e, :, cols], ring.at[s, 1], ring_sem.at[s, 1]))

    def expert_down(n, s):
        e, cols = lax.rem(n, n_pair) * 2, aligned(n // n_pair * WIDTH, WIDTH)
        return tuple(pltpu.make_async_copy(wd_hbm.at[e + i, :, cols], ring.at[s, i, 0:ff, :], ring_sem.at[s, i])
                     for i in range(2))

    def start(copies):
        for copy in copies:
            copy.start()

    def wait(copies):
        for copy in copies:
            copy.wait()

    def issue(n):
        s = lax.rem(n, DEPTH)

        @pl.when(n < n_s1)
        def _():
            start(shared_up(n, s))

        @pl.when(jnp.logical_and(n >= n_s1, n < first_g))
        def _():
            start(shared_down(n - n_s1, s))

        @pl.when(jnp.logical_and(n >= first_g, n < first_d))
        def _():
            start(expert_up(n - first_g, s))

        @pl.when(jnp.logical_and(n >= first_d, n < total))
        def _():
            start(expert_down(n - first_d, s))

    def remote(src, dst, send, recv, to):
        return pltpu.make_async_remote_copy(src_ref=src, dst_ref=dst, send_sem=send, recv_sem=recv,
                                            device_id={'ep': to}, device_id_type=MESH)

    def h_piece(owner, i):
        return hbuf.at[owner, i * piece:(i + 1) * piece, :]

    def send_h(i):
        return remote(h_piece(me, i), h_piece(me, i), h_send.at[i], h_recv.at[i], far)

    def take_h(i):
        return remote(h_piece(far, i), h_piece(far, i), h_send.at[i], h_recv.at[i], far)

    def send_sib():
        return remote(hbuf.at[me], hbuf.at[me], sib_send, sib_recv, sib)

    def take_sib():
        return remote(hbuf.at[sib], hbuf.at[sib], sib_send, sib_recv, sib)

    def pass_h(i):
        return remote(h_piece(far, i), h_piece(far, i), fwd_send.at[i], fwd_recv.at[i], sib)

    def take_passed(i):
        return remote(h_piece(diag, i), h_piece(diag, i), fwd_send.at[i], fwd_recv.at[i], sib)

    def three(buf, send, recv):
        mine = [remote(buf.at[me], buf.at[me], send.at[0], recv.at[0], far),
                remote(buf.at[me], buf.at[me], send.at[1], recv.at[1], sib),
                remote(buf.at[far], buf.at[far], send.at[2], recv.at[2], sib)]
        theirs = [remote(buf.at[far], buf.at[far], send.at[0], recv.at[0], far),
                  remote(buf.at[sib], buf.at[sib], send.at[1], recv.at[1], sib),
                  remote(buf.at[diag], buf.at[diag], send.at[2], recv.at[2], sib)]
        return mine, theirs

    idx_out, idx_in = three(idx_all, idx_send, idx_recv)
    p_out, p_in = three(prob, p_send, p_recv)

    load_x = pltpu.make_async_copy(x_hbm, hbuf.at[me], in_sem.at[0])
    load_x.start()
    load_r = pltpu.make_async_copy(wr_hbm, wr, in_sem.at[1])
    load_r.start()
    barrier = pltpu.get_barrier_semaphore()
    for peer in (sib, far):
        pl.semaphore_signal(barrier, inc=1, device_id={'ep': peer}, device_id_type=MESH)
    idx_all[me] = idx_ref[...]
    load_x.wait()
    start(shared_up(0, 0))
    start(shared_up(1, 1))
    pl.semaphore_wait(barrier, 2)
    idx_out[0].start()
    idx_out[1].start()

    gain = gain_ref[...].astype(F32).reshape(1, hidden)
    for i in range(PIECES):
        @pl.loop(0, piece // 32)
        def _(b):
            at = aligned(i * piece + b * 32, 32)
            x = hbuf[me, at, :].astype(F32)
            acc[at, :] = x
            inv_rms = lax.rsqrt(jnp.mean(x * x, axis=-1, keepdims=True) + 1e-6)
            hbuf[me, at, :] = (x * inv_rms * gain).astype(BF16)
        if i > 0:
            send_h(i - 1).start()
    for n in range(2, DEPTH):
        start(shared_up(n, n))
    send_h(PIECES - 1).start()
    send_sib().start()

    load_r.wait()
    logits = lax.dot_general(hbuf[me], wr[...], (((1,), (1,)), ((), ())), preferred_element_type=F32)
    prob[me] = jax.nn.softmax(logits, axis=-1)
    wsg = wsg_ref[...].astype(F32)

    @pl.loop(0, tok // 32)
    def _(b):
        at = aligned(b * 32, 32)
        dot = jnp.sum(hbuf[me, at, :].astype(F32) * wsg, axis=-1, keepdims=True)
        sgate[at, :] = jnp.broadcast_to(jax.nn.sigmoid(dot), (32, sgate.shape[1]))

    idx_in[0].wait_recv()
    idx_out[2].start()
    p_out[0].start()
    p_out[1].start()

    def shared_up_step(n):
        s = lax.rem(n, DEPTH)
        wait(shared_up(n, s))
        h = hbuf[me]
        gate = jnp.dot(h, ring[s, 0], preferred_element_type=F32)
        up = jnp.dot(h, ring[s, 1], preferred_element_type=F32)
        act[aligned(n // parts * tok, tok), aligned(lax.rem(n, parts) * WIDTH, WIDTH)] = (jax.nn.silu(gate) * up).astype(BF16)
        issue(n + DEPTH)

    @pl.loop(0, n_s1)
    def _(n):
        shared_up_step(n)

    def pass_on(i):
        take_h(i).wait_recv()
        pass_h(i).start()

    pass_on(0)

    @pl.loop(0, n_s2)
    def _(n):
        s = lax.rem(n_s1 + n, DEPTH)
        wait(shared_down(n, s))
        val = jnp.dot(act[0:tok, :], ring[s, 0, 0:ff, :], preferred_element_type=F32)
        val = val + jnp.dot(act[tok:2 * tok, :], ring[s, 1, 0:ff, :], preferred_element_type=F32)
        cols = aligned(n * WIDTH, WIDTH)
        acc[:, cols] = acc[:, cols] + sgate[:, 0:1] * val
        issue(n_s1 + n + DEPTH)

    pass_on(1)

    for copy in idx_in[1:]:
        copy.wait_recv()
    counts[...] = jnp.zeros_like(counts)
    before = lax.broadcasted_iota(jnp.int32, (tok, tok), 0) < lax.broadcasted_iota(jnp.int32, (tok, tok), 1)
    before = jnp.where(before, 1.0, 0.0).astype(BF16)
    expert_id = lax.broadcasted_iota(jnp.int32, (experts, tok), 0)
    for src in range(group):
        hit = expert_id == idx_all[src, 0:1, :]
        for k in range(1, top_k):
            hit = jnp.logical_or(hit, expert_id == idx_all[src, k:k + 1, :])
        chosen = jnp.where(hit, 1.0, 0.0).astype(F32)
        pos = jnp.dot(chosen.astype(BF16), before, preferred_element_type=F32)
        kept = jnp.logical_and(hit, pos + counts[:, 0:1] < capacity)
        post[src] = jnp.where(kept, pos, -1.0)
        counts[...] = counts[...] + jnp.broadcast_to(jnp.sum(chosen, axis=1, keepdims=True), counts.shape)

    place = lax.broadcasted_iota(jnp.int32, (local_max, tok), 0).astype(F32)

    @pl.loop(0, group)
    def _(src):
        for e in range(slots):
            row = post[src, pl.ds(me * slots + e, 1), :]
            act[aligned(src * width + e * local_max, local_max), 0:tok] = jnp.where(place == row, 1.0, 0.0).astype(BF16)

    def dispatch(src):
        @pl.loop(0, hidden // 256)
        def _(c):
            cols = aligned(c * 256, 256)
            got = jnp.dot(act[aligned(src * width, width), 0:tok], hbuf[src, :, cols], preferred_element_type=F32).astype(BF16)
            for e in range(slots):
                xbuf[aligned(e * rows + src * local_max, local_max), cols] = got[e * local_max:(e + 1) * local_max, :]

    dispatch(me)
    take_sib().wait_recv()
    dispatch(sib)
    for i in range(2, PIECES):
        pass_on(i)
    dispatch(far)
    for i in range(PIECES):
        take_passed(i).wait_recv()
    dispatch(diag)
    p_in[0].wait_recv()
    p_out[2].start()
    p_in[1].wait_recv()
    p_in[2].wait_recv()
    for i in range(PIECES):
        send_h(i).wait_send()
        pass_h(i).wait_send()
    send_sib().wait_send()
    for copy in idx_out + p_out:
        copy.wait_send()

    lane = lax.broadcasted_iota(jnp.int32, (experts, width), 1)
    scale = 65536 // local_max + 1
    slot_of = (lane * scale) // 65536
    spread = jnp.where(lax.broadcasted_iota(jnp.int32, (experts, width), 0) == slot_of + me * slots, 1.0, 0.0).astype(BF16)

    def gates(dst):
        col = lax.broadcasted_iota(jnp.int32, (1, width), 1)
        where = (col - (col * scale) // 65536 * local_max).astype(F32)
        here = lax.dot_general(post[dst].astype(BF16), spread, (((0,), (0,)), ((), ())), preferred_element_type=F32) == where
        rest = prob[dst]
        for i in range(3):
            part = rest.astype(BF16)
            rest = rest - part.astype(F32)
            val = jnp.where(here, jnp.dot(part, spread, preferred_element_type=F32), 0.0).astype(BF16)
            hbuf[dst, :, i * width:(i + 1) * width] = val

    @pl.loop(0, n_g)
    def _(n):
        s = lax.rem(first_g + n, DEPTH)
        wait(expert_up(n, s))
        at = aligned(n // parts * rows, rows)
        x = xbuf[at, :]
        gate = jnp.dot(x, ring[s, 0], preferred_element_type=F32)
        up = jnp.dot(x, ring[s, 1], preferred_element_type=F32)
        act[at, aligned(lax.rem(n, parts) * WIDTH, WIDTH)] = (jax.nn.silu(gate) * up).astype(BF16)
        issue(first_g + n + DEPTH)

        @pl.when(lax.rem(n, n_g // group) == n_g // group - 2)
        def _():
            gates(n // (n_g // group))

    def send_pair(j):
        return remote(pair, fromsib.at[lax.rem(j, 2)], pair_send, pair_recv.at[lax.rem(j, 2)], sib)

    def send_relay(j):
        return remote(relay.at[j], fromchip.at[j], relay_send.at[j], relay_recv.at[j], far)

    def hand_over(j):
        send_pair(j).wait()
        s = lax.rem(j, 2)
        cols = aligned(j * WIDTH, WIDTH)
        relay[j] = relay[j] + fromsib[s, 1]
        send_relay(j).start()
        acc[:, cols] = acc[:, cols] + fromsib[s, 0]

        @pl.when(j < n_chunk - 2)
        def _():
            pl.semaphore_signal(credit, inc=1, device_id={'ep': sib}, device_id_type=MESH)

    def combined(dst):
        mixed = xbuf[aligned(dst * width, width), 0:WIDTH]
        total = jnp.dot(hbuf[dst, :, 0:width], mixed, preferred_element_type=F32)
        for i in range(1, 3):
            total = total + jnp.dot(hbuf[dst, :, i * width:(i + 1) * width], mixed, preferred_element_type=F32)
        return total

    @pl.loop(0, n_d)
    def _(n):
        s = lax.rem(first_d + n, DEPTH)
        j, two = n // n_pair, lax.rem(n, n_pair)
        wait(expert_down(n, s))
        for i in range(2):
            e = two * 2 + i
            res = jnp.dot(act[aligned(e * rows, rows), :], ring[s, i, 0:ff, :], preferred_element_type=F32).astype(BF16)
            for dst in range(group):
                xbuf[aligned(dst * width + e * local_max, local_max), 0:WIDTH] = res[dst * local_max:(dst + 1) * local_max, :]
        issue(first_d + n + DEPTH)

        @pl.when(jnp.logical_and(two == 0, j > 0))
        def _():
            hand_over(j - 1)

        @pl.when(two == n_pair - 1)
        def _():
            pair[0] = combined(sib)
            pair[1] = combined(diag)

            @pl.when(j >= 2)
            def _():
                pl.semaphore_wait(credit, 1)

            send_pair(j).start()
            relay[j] = combined(far)
            cols = aligned(j * WIDTH, WIDTH)
            acc[:, cols] = acc[:, cols] + combined(me)

    hand_over(n_chunk - 1)

    def put(j):
        cols = aligned(j * WIDTH, WIDTH)
        return pltpu.make_async_copy(xbuf.at[0:tok, cols], out_hbm.at[:, cols], out_sem.at[j])

    @pl.loop(0, n_chunk)
    def _(j):
        cols = aligned(j * WIDTH, WIDTH)
        send_relay(j).wait()
        xbuf[0:tok, cols] = (acc[:, cols] + fromchip[j]).astype(BF16)
        put(j).start()

    @pl.loop(0, n_chunk)
    def _(j):
        put(j).wait()


def moe(hidden_in, idx_t, gain, w_router, wsg, s_gate, s_up, s_down, w_gate, w_up, w_down, group, capacity, local_max):
    tok, hidden = hidden_in.shape
    slots, _, ff = w_gate.shape
    experts = w_router.shape[0]
    rows = group * local_max
    chunks = hidden // WIDTH
    vmem, dma = pltpu.VMEM, pltpu.SemaphoreType.DMA
    hbm_spec, vmem_spec = pl.BlockSpec(memory_space=pl.ANY), pl.BlockSpec(memory_space=pltpu.VMEM)
    return pl.pallas_call(
        functools.partial(moe_kernel, group, experts, capacity, local_max),
        out_shape=jax.ShapeDtypeStruct((tok, hidden), BF16),
        in_specs=[hbm_spec, vmem_spec, vmem_spec, hbm_spec, vmem_spec] + [hbm_spec] * 6,
        out_specs=hbm_spec,
        scratch_shapes=[
            vmem((DEPTH, 2, hidden, WIDTH), BF16),
            vmem((slots * rows, hidden), BF16),
            vmem((slots * rows, ff), BF16),
            vmem((group, tok, hidden), BF16),
            vmem((2, tok, WIDTH), F32),
            vmem((chunks, tok, WIDTH), F32),
            vmem((2, 2, tok, WIDTH), F32),
            vmem((chunks, tok, WIDTH), F32),
            vmem((tok, hidden), F32),
            vmem((group, tok, experts), F32),
            vmem((group, experts, tok), F32),
            vmem((tok, 128), F32),
            vmem((group,) + idx_t.shape, jnp.int32),
            vmem((experts, hidden), BF16),
            vmem((experts, 128), F32),
            dma((DEPTH, 2)), dma((2,)), dma((chunks,)),
            dma((3,)), dma((3,)), dma((PIECES,)), dma((PIECES,)), dma, dma, dma((PIECES,)), dma((PIECES,)),
            dma((3,)), dma((3,)), dma, dma((2,)), dma((chunks,)), dma((chunks,)), pltpu.SemaphoreType.REGULAR,
        ],
        compiler_params=pltpu.CompilerParams(collective_id=0, has_side_effects=True, vmem_limit_bytes=67043328),
        cost_estimate=pl.CostEstimate(flops=6 * slots * rows * hidden * ff, bytes_accessed=6 * slots * hidden * ff, transcendentals=0),
        name="moe",
    )(hidden_in, idx_t, gain, w_router, wsg, s_gate, s_up, s_down, w_gate, w_up, w_down)


def solution(mesh):
    group = mesh.shape['ep']

    def device_block(hidden_in, topk_idx, norm_gain, w_router, w_sgate, s_gate, s_up, s_down, w_gate, w_up, w_down):
        tok_dev, hidden = hidden_in.shape
        top_k = topk_idx.shape[1]
        experts = w_router.shape[1]
        capacity = (5 * tok_dev * group * top_k + 4 * experts - 1) // (4 * experts)
        local_max = (2 * tok_dev * top_k + experts - 1) // experts
        return moe(hidden_in, topk_idx.T, norm_gain, w_router.T, w_sgate.reshape(1, hidden),
                   s_gate, s_up, s_down, w_gate, w_up, w_down, group, capacity, local_max)

    row_spec = P(('dp', 'ep'), None)
    full_spec = P(None, None)
    slot_spec = P('ep', None, None)
    in_specs = (row_spec, row_spec, P(None), full_spec, full_spec, full_spec, full_spec, full_spec,
                slot_spec, slot_spec, slot_spec)
    return jax.shard_map(device_block, mesh=mesh, in_specs=in_specs, out_specs=row_spec, check_vma=False)
```

```python
import functools

import jax
import jax.numpy as jnp
from jax import lax
from jax.experimental import pallas as pl
from jax.experimental.pallas import tpu as pltpu
from jax.sharding import PartitionSpec as P

F32 = jnp.float32
BF16 = jnp.bfloat16
MESH = pl.DeviceIdType.MESH
DEPTH = 4
WIDTH = 512
PIECES = 5
EARLY = 3
AHEAD = 8
CHUNK = 256


def aligned(start, size):
    return pl.ds(pl.multiple_of(start, size), size)


def moe_kernel(group, experts, capacity, local_max,
               x_hbm, idx_ref, gain_ref, wr_hbm, wsg_ref, sg_hbm, su_hbm, sd_hbm, wg_hbm, wu_hbm, wd_hbm,
               out_hbm,
               ring, xbuf, act, hbuf, work, acc, prob, post, sgate, idx_all, wr, counts,
               ring_sem, in_sem, out_sem, idx_send, idx_recv, h_send, h_recv, sib_send, sib_recv, fwd_send, fwd_recv,
               p_send, p_recv, pair_send, pair_recv, relay_send, relay_recv, credit, ready):
    tok, hidden = x_hbm.shape
    slots, _, ff = wg_hbm.shape
    top_k = idx_ref.shape[0]
    rows = group * local_max
    width = slots * local_max
    n_s1 = 2 * ff // WIDTH
    n_s2 = hidden // WIDTH
    parts = ff // WIDTH
    n_full = slots * parts - AHEAD
    n_chunk = hidden // CHUNK
    quads = slots // 4
    n_d = n_chunk * quads
    first_a = n_s1 + n_s2
    first_b, first_g = first_a + AHEAD, first_a + 2 * AHEAD
    first_d = first_g + n_full
    total = first_d + n_d
    piece = hidden // PIECES
    k_early = EARLY * piece

    me = lax.axis_index('ep')
    sib = me + 1 - 2 * lax.rem(me, 2)
    far = lax.rem(me + 2, group)
    diag = lax.rem(sib + 2, group)

    def shared_up(n, s):
        cols = aligned(n * WIDTH, WIDTH)
        return (pltpu.make_async_copy(sg_hbm.at[:, cols], ring.at[s, 0], ring_sem.at[s, 0]),
                pltpu.make_async_copy(su_hbm.at[:, cols], ring.at[s, 1], ring_sem.at[s, 1]))

    def shared_down(n, s):
        cols = aligned(n * WIDTH, WIDTH)
        return tuple(pltpu.make_async_copy(sd_hbm.at[i * ff:(i + 1) * ff, cols], ring.at[s, i, 0:ff, :], ring_sem.at[s, i])
                     for i in range(2))

    def expert_up(n, s, low=0, high=hidden):
        e, cols = n // parts, aligned(lax.rem(n, parts) * WIDTH, WIDTH)
        return tuple(pltpu.make_async_copy(w.at[e, low:high, cols], ring.at[s, i, 0:high - low, :], ring_sem.at[s, i])
                     for i, w in enumerate((wg_hbm, wu_hbm)))

    def expert_down(n, s):
        e, cols = lax.rem(n, quads) * 4, aligned(n // quads * CHUNK, CHUNK)
        return tuple(pltpu.make_async_copy(wd_hbm.at[e + i, :, cols], down_part(s, i), ring_sem.at[s, i]) for i in range(4))

    def down_part(s, i):
        return ring.at[s, i // 2, 0:ff, i % 2 * CHUNK:(i % 2 + 1) * CHUNK]

    def start(copies):
        for copy in copies:
            copy.start()

    def wait(copies):
        for copy in copies:
            copy.wait()

    def issue(n):
        s = lax.rem(n, DEPTH)

        @pl.when(n < n_s1)
        def _():
            start(shared_up(n, s))

        @pl.when(jnp.logical_and(n >= n_s1, n < first_a))
        def _():
            start(shared_down(n - n_s1, s))

        @pl.when(jnp.logical_and(n >= first_a, n < first_b))
        def _():
            start(expert_up(n - first_a, s, 0, k_early))

        @pl.when(jnp.logical_and(n >= first_b, n < first_g))
        def _():
            start(expert_up(n - first_b, s, k_early, hidden))

        @pl.when(jnp.logical_and(n >= first_g, n < first_d))
        def _():
            start(expert_up(n - first_g + AHEAD, s))

        @pl.when(jnp.logical_and(n >= first_d, n < total))
        def _():
            start(expert_down(n - first_d, s))

    def remote(src, dst, send, recv, to):
        return pltpu.make_async_remote_copy(src_ref=src, dst_ref=dst, send_sem=send, recv_sem=recv,
                                            device_id={'ep': to}, device_id_type=MESH)

    def h_piece(owner, i):
        return hbuf.at[owner, :, i * piece:(i + 1) * piece]

    def send_h(i):
        return remote(h_piece(me, i), h_piece(me, i), h_send.at[i], h_recv.at[i], far)

    def take_h(i):
        return remote(h_piece(far, i), h_piece(far, i), h_send.at[i], h_recv.at[i], far)

    def send_sib():
        return remote(hbuf.at[me], hbuf.at[me], sib_send, sib_recv, sib)

    def take_sib():
        return remote(hbuf.at[sib], hbuf.at[sib], sib_send, sib_recv, sib)

    def pass_h(i):
        return remote(h_piece(far, i), h_piece(far, i), fwd_send.at[i], fwd_recv.at[i], sib)

    def take_passed(i):
        return remote(h_piece(diag, i), h_piece(diag, i), fwd_send.at[i], fwd_recv.at[i], sib)

    def three(buf, send, recv):
        mine = [remote(buf.at[me], buf.at[me], send.at[0], recv.at[0], far),
                remote(buf.at[me], buf.at[me], send.at[1], recv.at[1], sib),
                remote(buf.at[far], buf.at[far], send.at[2], recv.at[2], sib)]
        theirs = [remote(buf.at[far], buf.at[far], send.at[0], recv.at[0], far),
                  remote(buf.at[sib], buf.at[sib], send.at[1], recv.at[1], sib),
                  remote(buf.at[diag], buf.at[diag], send.at[2], recv.at[2], sib)]
        return mine, theirs

    idx_out, idx_in = three(idx_all, idx_send, idx_recv)
    p_out, p_in = three(prob, p_send, p_recv)

    load_x = pltpu.make_async_copy(x_hbm, hbuf.at[me], in_sem.at[0])
    load_x.start()
    load_r = pltpu.make_async_copy(wr_hbm, wr, in_sem.at[1])
    load_r.start()
    barrier = pltpu.get_barrier_semaphore()
    for peer in (sib, far):
        pl.semaphore_signal(barrier, inc=1, device_id={'ep': peer}, device_id_type=MESH)
    idx_all[me] = idx_ref[...]
    load_x.wait()
    start(shared_up(0, 0))
    start(shared_up(1, 1))
    pl.semaphore_wait(barrier, 2)
    idx_out[0].start()
    idx_out[1].start()

    @pl.loop(0, tok // 32)
    def _(b):
        at = aligned(b * 32, 32)
        x = hbuf[me, at, :].astype(F32)
        acc[at, :] = x
        inv_rms = lax.rsqrt(jnp.mean(x * x, axis=-1, keepdims=True) + 1e-6)
        sgate[at, :] = jnp.broadcast_to(inv_rms, (32, sgate.shape[1]))

    gain = gain_ref[...].astype(F32).reshape(1, hidden)
    for i in range(PIECES):
        cols = slice(i * piece, (i + 1) * piece)

        @pl.loop(0, tok // 64)
        def _(b):
            at = aligned(b * 64, 64)
            hbuf[me, at, cols] = (acc[at, cols] * sgate[at, 0:1] * gain[:, cols]).astype(BF16)
        if i > 0:
            send_h(i - 1).start()
    for n in range(2, DEPTH):
        start(shared_up(n, n))
    send_h(PIECES - 1).start()
    send_sib().start()

    wsg = wsg_ref[...].astype(F32)

    @pl.loop(0, tok // 32)
    def _(b):
        at = aligned(b * 32, 32)
        dot = jnp.sum(hbuf[me, at, :].astype(F32) * wsg, axis=-1, keepdims=True)
        sgate[at, :] = jnp.broadcast_to(jax.nn.sigmoid(dot), (32, sgate.shape[1]))

    idx_in[0].wait_recv()
    idx_out[2].start()

    def shared_up_step(n):
        s = lax.rem(n, DEPTH)
        wait(shared_up(n, s))
        h = hbuf[me]
        gate = jnp.dot(h, ring[s, 0], preferred_element_type=F32)
        up = jnp.dot(h, ring[s, 1], preferred_element_type=F32)
        act[aligned(n // parts * tok, tok), aligned(lax.rem(n, parts) * WIDTH, WIDTH)] = (jax.nn.silu(gate) * up).astype(BF16)
        issue(n + DEPTH)

    @pl.loop(0, n_s1)
    def _(n):
        shared_up_step(n)

    def pass_on(i):
        take_h(i).wait_recv()
        pass_h(i).start()

    pass_on(0)

    @pl.loop(0, n_s2)
    def _(n):
        s = lax.rem(n_s1 + n, DEPTH)
        wait(shared_down(n, s))
        val = jnp.dot(act[0:tok, :], ring[s, 0, 0:ff, :], preferred_element_type=F32)
        val = val + jnp.dot(act[tok:2 * tok, :], ring[s, 1, 0:ff, :], preferred_element_type=F32)
        cols = aligned(n * WIDTH, WIDTH)
        acc[:, cols] = acc[:, cols] + sgate[:, 0:1] * val
        issue(n_s1 + n + DEPTH)

    pass_on(1)

    for copy in idx_in[1:]:
        copy.wait_recv()
    counts[...] = jnp.zeros_like(counts)
    before = lax.broadcasted_iota(jnp.int32, (tok, tok), 0) < lax.broadcasted_iota(jnp.int32, (tok, tok), 1)
    before = jnp.where(before, 1.0, 0.0).astype(BF16)
    expert_id = lax.broadcasted_iota(jnp.int32, (experts, tok), 0)
    for src in range(group):
        hit = expert_id == idx_all[src, 0:1, :]
        for k in range(1, top_k):
            hit = jnp.logical_or(hit, expert_id == idx_all[src, k:k + 1, :])
        chosen = jnp.where(hit, 1.0, 0.0).astype(F32)
        pos = jnp.dot(chosen.astype(BF16), before, preferred_element_type=F32)
        kept = jnp.logical_and(hit, pos + counts[:, 0:1] < capacity)
        post[src] = jnp.where(kept, pos, -1.0)
        counts[...] = counts[...] + jnp.broadcast_to(jnp.sum(chosen, axis=1, keepdims=True), counts.shape)

    place = lax.broadcasted_iota(jnp.int32, (local_max, tok), 0).astype(F32)

    @pl.loop(0, group)
    def _(src):
        for e in range(slots):
            row = post[src, pl.ds(me * slots + e, 1), :]
            act[aligned(src * width + e * local_max, local_max), 0:tok] = jnp.where(place == row, 1.0, 0.0).astype(BF16)

    def dispatch(src, low, high, step=1):
        @pl.loop(low // step, high // step)
        def _(c):
            cols = aligned(c * step * piece, step * piece)
            for first in range(0, slots, 4):
                pick = act[aligned(src * width + first * local_max, 4 * local_max), 0:tok]
                got = jnp.dot(pick, hbuf[src, :, cols], preferred_element_type=F32).astype(BF16)
                for e in range(4):
                    xbuf[aligned((first + e) * rows + src * local_max, local_max), cols] = got[e * local_max:(e + 1) * local_max, :]

    def rows_of(u):
        return aligned(u // parts * rows, rows)

    def expert_a(u):
        s = lax.rem(first_a + u, DEPTH)
        wait(expert_up(u, s, 0, k_early))
        x = xbuf[rows_of(u), 0:k_early]
        for i in range(2):
            res = jnp.dot(x, ring[s, i, 0:k_early, :], preferred_element_type=F32)
            for half in range(2):
                work[4 * u + 2 * i + half, 0:rows, :] = res[:, half * CHUNK:(half + 1) * CHUNK]
        issue(first_a + u + DEPTH)

    dispatch(me, 0, PIECES)
    take_sib().wait_recv()
    dispatch(sib, 0, PIECES)
    for i in range(2, EARLY):
        pass_on(i)
    dispatch(far, 0, EARLY)
    for i in range(EARLY):
        take_passed(i).wait_recv()
    dispatch(diag, 0, EARLY)

    @pl.loop(0, AHEAD // 2)
    def _(u):
        expert_a(u)

    pass_on(EARLY)
    dispatch(far, EARLY, EARLY + 1)

    @pl.loop(AHEAD // 2, AHEAD)
    def _(u):
        expert_a(u)

    take_passed(EARLY).wait_recv()
    dispatch(diag, EARLY, EARLY + 1)
    pass_on(EARLY + 1)
    dispatch(far, EARLY + 1, PIECES)
    take_passed(EARLY + 1).wait_recv()
    dispatch(diag, EARLY + 1, PIECES)

    @pl.loop(0, AHEAD)
    def _(u):
        s = lax.rem(first_b + u, DEPTH)
        wait(expert_up(u, s, k_early, hidden))
        x = xbuf[rows_of(u), k_early:hidden]
        gate = jnp.dot(x, ring[s, 0, 0:hidden - k_early, :], preferred_element_type=F32)
        up = jnp.dot(x, ring[s, 1, 0:hidden - k_early, :], preferred_element_type=F32)
        for half in range(2):
            cols = slice(half * CHUNK, (half + 1) * CHUNK)
            g = work[4 * u + half, 0:rows, :] + gate[:, cols]
            v = work[4 * u + 2 + half, 0:rows, :] + up[:, cols]
            act[rows_of(u), aligned(lax.rem(u, parts) * WIDTH + half * CHUNK, CHUNK)] = (jax.nn.silu(g) * v).astype(BF16)
        issue(first_b + u + DEPTH)

    pl.semaphore_signal(credit, inc=2, device_id={'ep': sib}, device_id_type=MESH)
    pl.semaphore_signal(ready, inc=1, device_id={'ep': far}, device_id_type=MESH)
    for i in range(PIECES):
        send_h(i).wait_send()
        pass_h(i).wait_send()
    send_sib().wait_send()
    for copy in idx_out:
        copy.wait_send()

    lane = lax.broadcasted_iota(jnp.int32, (experts, width), 1)
    scale = 65536 // local_max + 1
    slot_of = (lane * scale) // 65536
    spread = jnp.where(lax.broadcasted_iota(jnp.int32, (experts, width), 0) == slot_of + me * slots, 1.0, 0.0).astype(BF16)

    def gates(dst):
        col = lax.broadcasted_iota(jnp.int32, (1, width), 1)
        where = (col - (col * scale) // 65536 * local_max).astype(F32)
        here = lax.dot_general(post[dst].astype(BF16), spread, (((0,), (0,)), ((), ())), preferred_element_type=F32) == where
        rest = prob[dst]
        for i in range(3):
            part = rest.astype(BF16)
            rest = rest - part.astype(F32)
            val = jnp.where(here, jnp.dot(part, spread, preferred_element_type=F32), 0.0).astype(BF16)
            hbuf[dst, :, i * width:(i + 1) * width] = val

    @pl.loop(0, n_full)
    def _(n):
        s = lax.rem(first_g + n, DEPTH)
        u = n + AHEAD
        wait(expert_up(u, s))
        x = xbuf[rows_of(u), :]
        gate = jnp.dot(x, ring[s, 0], preferred_element_type=F32)
        up = jnp.dot(x, ring[s, 1], preferred_element_type=F32)
        act[rows_of(u), aligned(lax.rem(u, parts) * WIDTH, WIDTH)] = (jax.nn.silu(gate) * up).astype(BF16)
        issue(first_g + n + DEPTH)

        @pl.when(n == 0)
        def _():
            load_r.wait()
            logits = lax.dot_general(hbuf[me], wr[...], (((1,), (1,)), ((), ())), preferred_element_type=F32)
            prob[me] = jax.nn.softmax(logits, axis=-1)

        @pl.when(n == 1)
        def _():
            p_out[0].start()
            p_out[1].start()

        @pl.when(n == 4)
        def _():
            p_in[0].wait_recv()
            p_out[2].start()

        @pl.when(n == 6)
        def _():
            for copy in p_in[1:]:
                copy.wait_recv()
            for copy in p_out:
                copy.wait_send()

        @pl.when(lax.rem(n, n_full // group) == n_full // group - 2)
        def _():
            gates(n // (n_full // group))

    def send_pair(j):
        at = 2 * n_chunk
        return remote(work.at[at + 4:at + 6], work.at[pl.ds(at + 2 * lax.rem(j, 2), 2)], pair_send, pair_recv.at[lax.rem(j, 2)], sib)

    def send_relay(j):
        return remote(work.at[j], work.at[n_chunk + j], relay_send.at[j], relay_recv.at[j], far)

    def hand_over(j):
        send_pair(j).wait()
        got = 2 * n_chunk + 2 * lax.rem(j, 2)
        cols = aligned(j * CHUNK, CHUNK)
        work[j] = work[j] + work[got + 1]
        acc[:, cols] = acc[:, cols] + work[got]

        @pl.when(j == 0)
        def _():
            pl.semaphore_wait(ready, 1)

        send_relay(j).start()

        @pl.when(j < n_chunk - 2)
        def _():
            pl.semaphore_signal(credit, inc=1, device_id={'ep': sib}, device_id_type=MESH)

    def combined(dst):
        mixed = xbuf[aligned(dst * width, width), 0:CHUNK]
        total = jnp.dot(hbuf[dst, :, 0:width], mixed, preferred_element_type=F32)
        for i in range(1, 3):
            total = total + jnp.dot(hbuf[dst, :, i * width:(i + 1) * width], mixed, preferred_element_type=F32)
        return total

    @pl.loop(0, n_d)
    def _(n):
        s = lax.rem(first_d + n, DEPTH)
        j, quad = n // quads, lax.rem(n, quads)
        wait(expert_down(n, s))
        for i in range(4):
            e = quad * 4 + i
            res = jnp.dot(act[aligned(e * rows, rows), :], down_part(s, i)[...], preferred_element_type=F32).astype(BF16)
            for dst in range(group):
                xbuf[aligned(dst * width + e * local_max, local_max), 0:CHUNK] = res[dst * local_max:(dst + 1) * local_max, :]
        issue(first_d + n + DEPTH)

        @pl.when(jnp.logical_and(quad == 0, j > 1))
        def _():
            hand_over(j - 1)

        @pl.when(quad == quads - 1)
        def _():
            work[2 * n_chunk + 4] = combined(sib)
            work[2 * n_chunk + 5] = combined(diag)
            pl.semaphore_wait(credit, 1)
            send_pair(j).start()
            work[j] = combined(far)
            cols = aligned(j * CHUNK, CHUNK)
            acc[:, cols] = acc[:, cols] + combined(me)

            @pl.when(j == 0)
            def _():
                hand_over(0)

    hand_over(n_chunk - 1)

    def put(j):
        cols = aligned(j * CHUNK, CHUNK)
        return pltpu.make_async_copy(xbuf.at[0:tok, cols], out_hbm.at[:, cols], out_sem.at[j])

    @pl.loop(0, n_chunk)
    def _(j):
        cols = aligned(j * CHUNK, CHUNK)
        send_relay(j).wait()
        xbuf[0:tok, cols] = (acc[:, cols] + work[n_chunk + j]).astype(BF16)
        put(j).start()

    @pl.loop(0, n_chunk)
    def _(j):
        put(j).wait()


def moe(hidden_in, idx_t, gain, w_router, wsg, s_gate, s_up, s_down, w_gate, w_up, w_down, group, capacity, local_max):
    tok, hidden = hidden_in.shape
    slots, _, ff = w_gate.shape
    experts = w_router.shape[0]
    rows = group * local_max
    chunks = hidden // CHUNK
    vmem, dma = pltpu.VMEM, pltpu.SemaphoreType.DMA
    hbm_spec, vmem_spec = pl.BlockSpec(memory_space=pl.ANY), pl.BlockSpec(memory_space=pltpu.VMEM)
    return pl.pallas_call(
        functools.partial(moe_kernel, group, experts, capacity, local_max),
        out_shape=jax.ShapeDtypeStruct((tok, hidden), BF16),
        in_specs=[hbm_spec, vmem_spec, vmem_spec, hbm_spec, vmem_spec] + [hbm_spec] * 6,
        out_specs=hbm_spec,
        scratch_shapes=[
            vmem((DEPTH, 2, hidden, WIDTH), BF16),
            vmem((slots * rows, hidden), BF16),
            vmem((slots * rows, ff), BF16),
            vmem((group, tok, hidden), BF16),
            vmem((max(2 * chunks + 6, 4 * AHEAD), tok, CHUNK), F32),
            vmem((tok, hidden), F32),
            vmem((group, tok, experts), F32),
            vmem((group, experts, tok), F32),
            vmem((tok, 128), F32),
            vmem((group,) + idx_t.shape, jnp.int32),
            vmem((experts, hidden), BF16),
            vmem((experts, 128), F32),
            dma((DEPTH, 4)), dma((2,)), dma((chunks,)),
            dma((3,)), dma((3,)), dma((PIECES,)), dma((PIECES,)), dma, dma, dma((PIECES,)), dma((PIECES,)),
            dma((3,)), dma((3,)), dma, dma((2,)), dma((chunks,)), dma((chunks,)), pltpu.SemaphoreType.REGULAR, pltpu.SemaphoreType.REGULAR,
        ],
        compiler_params=pltpu.CompilerParams(collective_id=0, has_side_effects=True, vmem_limit_bytes=67043328),
        cost_estimate=pl.CostEstimate(flops=6 * slots * rows * hidden * ff, bytes_accessed=6 * slots * hidden * ff, transcendentals=0),
        name="moe",
    )(hidden_in, idx_t, gain, w_router, wsg, s_gate, s_up, s_down, w_gate, w_up, w_down)


def solution(mesh):
    group = mesh.shape['ep']

    def device_block(hidden_in, topk_idx, norm_gain, w_router, w_sgate, s_gate, s_up, s_down, w_gate, w_up, w_down):
        tok_dev, hidden = hidden_in.shape
        top_k = topk_idx.shape[1]
        experts = w_router.shape[1]
        capacity = (5 * tok_dev * group * top_k + 4 * experts - 1) // (4 * experts)
        local_max = (2 * tok_dev * top_k + experts - 1) // experts
        return moe(hidden_in, topk_idx.T, norm_gain, w_router.T, w_sgate.reshape(1, hidden),
                   s_gate, s_up, s_down, w_gate, w_up, w_down, group, capacity, local_max)

    row_spec = P(('dp', 'ep'), None)
    full_spec = P(None, None)
    slot_spec = P('ep', None, None)
    in_specs = (row_spec, row_spec, P(None), full_spec, full_spec, full_spec, full_spec, full_spec,
                slot_spec, slot_spec, slot_spec)
    return jax.shard_map(device_block, mesh=mesh, in_specs=in_specs, out_specs=row_spec, check_vma=False)
```

```python
import functools

import jax
import jax.numpy as jnp
from jax import lax
from jax.experimental import pallas as pl
from jax.experimental.pallas import tpu as pltpu
from jax.sharding import PartitionSpec as P

F32 = jnp.float32
BF16 = jnp.bfloat16
MESH = pl.DeviceIdType.MESH
DEPTH = 4
WIDTH = 512
PIECES = 5
EARLY = 3
AHEAD = 8
BETWEEN = 4
CHUNK = 256


def aligned(start, size):
    return pl.ds(pl.multiple_of(start, size), size)


def moe_kernel(group, experts, capacity, local_max,
               x_hbm, idx_ref, gain_ref, wr_hbm, wsg_ref, sg_hbm, su_hbm, sd_hbm, wg_hbm, wu_hbm, wd_hbm,
               out_hbm,
               ring, xbuf, act, hbuf, work, acc, prob, post, sgate, idx_all, wr, counts,
               ring_sem, in_sem, out_sem, idx_send, idx_recv, h_send, h_recv, sib_send, sib_recv, fwd_send, fwd_recv,
               p_send, p_recv, pair_send, pair_recv, relay_send, relay_recv, credit, ready):
    tok, hidden = x_hbm.shape
    slots, _, ff = wg_hbm.shape
    top_k = idx_ref.shape[0]
    rows = group * local_max
    width = slots * local_max
    n_s1 = 2 * ff // WIDTH
    n_s2 = hidden // WIDTH
    parts = ff // WIDTH
    n_full = slots * parts - AHEAD
    n_chunk = hidden // CHUNK
    quads = slots // 4
    n_d = n_chunk * quads
    first_a = n_s1 + n_s2
    first_m = first_a + AHEAD
    first_b = first_m + BETWEEN
    first_g = first_b + AHEAD
    first_d = first_g + n_full - BETWEEN
    total = first_d + n_d
    piece = hidden // PIECES
    k_early = EARLY * piece

    me = lax.axis_index('ep')
    sib = me + 1 - 2 * lax.rem(me, 2)
    far = lax.rem(me + 2, group)
    diag = lax.rem(sib + 2, group)

    def shared_up(n, s):
        cols = aligned(n * WIDTH, WIDTH)
        return (pltpu.make_async_copy(sg_hbm.at[:, cols], ring.at[s, 0], ring_sem.at[s, 0]),
                pltpu.make_async_copy(su_hbm.at[:, cols], ring.at[s, 1], ring_sem.at[s, 1]))

    def shared_down(n, s):
        cols = aligned(n * WIDTH, WIDTH)
        return tuple(pltpu.make_async_copy(sd_hbm.at[i * ff:(i + 1) * ff, cols], ring.at[s, i, 0:ff, :], ring_sem.at[s, i])
                     for i in range(2))

    def expert_up(n, s, low=0, high=hidden):
        e, cols = n // parts, aligned(lax.rem(n, parts) * WIDTH, WIDTH)
        return tuple(pltpu.make_async_copy(w.at[e, low:high, cols], ring.at[s, i, 0:high - low, :], ring_sem.at[s, i])
                     for i, w in enumerate((wg_hbm, wu_hbm)))

    def expert_down(n, s):
        e, cols = lax.rem(n, quads) * 4, aligned(n // quads * CHUNK, CHUNK)
        return tuple(pltpu.make_async_copy(wd_hbm.at[e + i, :, cols], down_part(s, i), ring_sem.at[s, i]) for i in range(4))

    def down_part(s, i):
        return ring.at[s, i // 2, 0:ff, i % 2 * CHUNK:(i % 2 + 1) * CHUNK]

    def start(copies):
        for copy in copies:
            copy.start()

    def wait(copies):
        for copy in copies:
            copy.wait()

    def issue(n):
        s = lax.rem(n, DEPTH)

        @pl.when(n < n_s1)
        def _():
            start(shared_up(n, s))

        @pl.when(jnp.logical_and(n >= n_s1, n < first_a))
        def _():
            start(shared_down(n - n_s1, s))

        @pl.when(jnp.logical_and(n >= first_a, n < first_m))
        def _():
            start(expert_up(n - first_a, s, 0, k_early))

        @pl.when(jnp.logical_and(n >= first_m, n < first_b))
        def _():
            start(expert_up(n - first_m + AHEAD, s))

        @pl.when(jnp.logical_and(n >= first_b, n < first_g))
        def _():
            start(expert_up(n - first_b, s, k_early, hidden))

        @pl.when(jnp.logical_and(n >= first_g, n < first_d))
        def _():
            start(expert_up(n - first_g + BETWEEN + AHEAD, s))

        @pl.when(jnp.logical_and(n >= first_d, n < total))
        def _():
            start(expert_down(n - first_d, s))

    def remote(src, dst, send, recv, to):
        return pltpu.make_async_remote_copy(src_ref=src, dst_ref=dst, send_sem=send, recv_sem=recv,
                                            device_id={'ep': to}, device_id_type=MESH)

    def h_piece(owner, i):
        return hbuf.at[owner, :, i * piece:(i + 1) * piece]

    def send_h(i):
        return remote(h_piece(me, i), h_piece(me, i), h_send.at[i], h_recv.at[i], far)

    def take_h(i):
        return remote(h_piece(far, i), h_piece(far, i), h_send.at[i], h_recv.at[i], far)

    def send_sib():
        return remote(hbuf.at[me], hbuf.at[me], sib_send, sib_recv, sib)

    def take_sib():
        return remote(hbuf.at[sib], hbuf.at[sib], sib_send, sib_recv, sib)

    def pass_h(i):
        return remote(h_piece(far, i), h_piece(far, i), fwd_send.at[i], fwd_recv.at[i], sib)

    def take_passed(i):
        return remote(h_piece(diag, i), h_piece(diag, i), fwd_send.at[i], fwd_recv.at[i], sib)

    def three(buf, send, recv):
        mine = [remote(buf.at[me], buf.at[me], send.at[0], recv.at[0], far),
                remote(buf.at[me], buf.at[me], send.at[1], recv.at[1], sib),
                remote(buf.at[far], buf.at[far], send.at[2], recv.at[2], sib)]
        theirs = [remote(buf.at[far], buf.at[far], send.at[0], recv.at[0], far),
                  remote(buf.at[sib], buf.at[sib], send.at[1], recv.at[1], sib),
                  remote(buf.at[diag], buf.at[diag], send.at[2], recv.at[2], sib)]
        return mine, theirs

    idx_out, idx_in = three(idx_all, idx_send, idx_recv)
    p_out, p_in = three(prob, p_send, p_recv)

    load_x = pltpu.make_async_copy(x_hbm, hbuf.at[me], in_sem.at[0])
    load_x.start()
    load_r = pltpu.make_async_copy(wr_hbm, wr, in_sem.at[1])
    load_r.start()
    barrier = pltpu.get_barrier_semaphore()
    for peer in (sib, far):
        pl.semaphore_signal(barrier, inc=1, device_id={'ep': peer}, device_id_type=MESH)
    idx_all[me] = idx_ref[...]
    load_x.wait()
    start(shared_up(0, 0))
    start(shared_up(1, 1))
    pl.semaphore_wait(barrier, 2)
    idx_out[0].start()
    idx_out[1].start()

    @pl.loop(0, tok // 64)
    def _(b):
        at = aligned(b * 64, 64)
        x = hbuf[me, at, :].astype(F32)
        acc[at, :] = x
        inv_rms = lax.rsqrt(jnp.mean(x * x, axis=-1, keepdims=True) + 1e-6)
        sgate[at, :] = jnp.broadcast_to(inv_rms, (64, sgate.shape[1]))

    gain = gain_ref[...].astype(F32).reshape(1, hidden)
    for i in range(PIECES):
        cols = slice(i * piece, (i + 1) * piece)

        @pl.loop(0, tok // 64)
        def _(b):
            at = aligned(b * 64, 64)
            hbuf[me, at, cols] = (acc[at, cols] * sgate[at, 0:1] * gain[:, cols]).astype(BF16)
        if i > 0:
            send_h(i - 1).start()
    for n in range(2, DEPTH):
        start(shared_up(n, n))
    send_h(PIECES - 1).start()
    send_sib().start()

    wsg = wsg_ref[...].astype(F32)

    @pl.loop(0, tok // 32)
    def _(b):
        at = aligned(b * 32, 32)
        dot = jnp.sum(hbuf[me, at, :].astype(F32) * wsg, axis=-1, keepdims=True)
        sgate[at, :] = jnp.broadcast_to(jax.nn.sigmoid(dot), (32, sgate.shape[1]))

    idx_in[0].wait_recv()
    idx_out[2].start()

    def shared_up_step(n):
        s = lax.rem(n, DEPTH)
        wait(shared_up(n, s))
        h = hbuf[me]
        gate = jnp.dot(h, ring[s, 0], preferred_element_type=F32)
        up = jnp.dot(h, ring[s, 1], preferred_element_type=F32)
        act[aligned(n // parts * tok, tok), aligned(lax.rem(n, parts) * WIDTH, WIDTH)] = (jax.nn.silu(gate) * up).astype(BF16)
        issue(n + DEPTH)

    @pl.loop(0, n_s1)
    def _(n):
        shared_up_step(n)

    def pass_on(i):
        take_h(i).wait_recv()
        pass_h(i).start()

    pass_on(0)

    @pl.loop(0, n_s2)
    def _(n):
        s = lax.rem(n_s1 + n, DEPTH)
        wait(shared_down(n, s))
        val = jnp.dot(act[0:tok, :], ring[s, 0, 0:ff, :], preferred_element_type=F32)
        val = val + jnp.dot(act[tok:2 * tok, :], ring[s, 1, 0:ff, :], preferred_element_type=F32)
        cols = aligned(n * WIDTH, WIDTH)
        acc[:, cols] = acc[:, cols] + sgate[:, 0:1] * val
        issue(n_s1 + n + DEPTH)

    pass_on(1)

    for copy in idx_in[1:]:
        copy.wait_recv()
    counts[...] = jnp.zeros_like(counts)
    before = lax.broadcasted_iota(jnp.int32, (tok, tok), 0) < lax.broadcasted_iota(jnp.int32, (tok, tok), 1)
    before = jnp.where(before, 1.0, 0.0).astype(BF16)
    expert_id = lax.broadcasted_iota(jnp.int32, (experts, tok), 0)
    for src in range(group):
        hit = expert_id == idx_all[src, 0:1, :]
        for k in range(1, top_k):
            hit = jnp.logical_or(hit, expert_id == idx_all[src, k:k + 1, :])
        chosen = jnp.where(hit, 1.0, 0.0).astype(F32)
        pos = jnp.dot(chosen.astype(BF16), before, preferred_element_type=F32)
        kept = jnp.logical_and(hit, pos + counts[:, 0:1] < capacity)
        post[src] = jnp.where(kept, pos, -1.0)
        counts[...] = counts[...] + jnp.broadcast_to(jnp.sum(chosen, axis=1, keepdims=True), counts.shape)

    place = lax.broadcasted_iota(jnp.int32, (local_max, tok), 0).astype(F32)

    @pl.loop(0, group)
    def _(src):
        for e in range(slots):
            row = post[src, pl.ds(me * slots + e, 1), :]
            act[aligned(src * width + e * local_max, local_max), 0:tok] = jnp.where(place == row, 1.0, 0.0).astype(BF16)

    def dispatch(src, low, high, step=1):
        @pl.loop(low // step, high // step)
        def _(c):
            cols = aligned(c * step * piece, step * piece)
            for first in range(0, slots, 4):
                pick = act[aligned(src * width + first * local_max, 4 * local_max), 0:tok]
                got = jnp.dot(pick, hbuf[src, :, cols], preferred_element_type=F32).astype(BF16)
                for e in range(4):
                    xbuf[aligned((first + e) * rows + src * local_max, local_max), cols] = got[e * local_max:(e + 1) * local_max, :]

    def rows_of(u):
        return aligned(u // parts * rows, rows)

    def expert_a(u):
        s = lax.rem(first_a + u, DEPTH)
        wait(expert_up(u, s, 0, k_early))
        x = xbuf[rows_of(u), 0:k_early]
        for i in range(2):
            res = jnp.dot(x, ring[s, i, 0:k_early, :], preferred_element_type=F32)
            for half in range(2):
                work[4 * u + 2 * i + half, 0:rows, :] = res[:, half * CHUNK:(half + 1) * CHUNK]
        issue(first_a + u + DEPTH)

    dispatch(me, 0, PIECES)
    take_sib().wait_recv()
    dispatch(sib, 0, PIECES)
    for i in range(2, EARLY):
        pass_on(i)
    dispatch(far, 0, EARLY)
    for i in range(EARLY):
        take_passed(i).wait_recv()
    dispatch(diag, 0, EARLY)

    @pl.loop(0, AHEAD // 2)
    def _(u):
        expert_a(u)

    pass_on(EARLY)
    dispatch(far, EARLY, EARLY + 1)

    @pl.loop(AHEAD // 2, AHEAD)
    def _(u):
        expert_a(u)

    take_passed(EARLY).wait_recv()
    dispatch(diag, EARLY, EARLY + 1)
    pass_on(EARLY + 1)
    dispatch(far, EARLY + 1, PIECES)
    take_passed(EARLY + 1).wait_recv()
    dispatch(diag, EARLY + 1, PIECES)

    lane = lax.broadcasted_iota(jnp.int32, (experts, width), 1)
    scale = 65536 // local_max + 1
    slot_of = (lane * scale) // 65536
    spread = jnp.where(lax.broadcasted_iota(jnp.int32, (experts, width), 0) == slot_of + me * slots, 1.0, 0.0).astype(BF16)

    def gates(dst):
        col = lax.broadcasted_iota(jnp.int32, (1, width), 1)
        where = (col - (col * scale) // 65536 * local_max).astype(F32)
        here = lax.dot_general(post[dst].astype(BF16), spread, (((0,), (0,)), ((), ())), preferred_element_type=F32) == where
        rest = prob[dst]
        for i in range(3):
            part = rest.astype(BF16)
            rest = rest - part.astype(F32)
            val = jnp.where(here, jnp.dot(part, spread, preferred_element_type=F32), 0.0).astype(BF16)
            hbuf[dst, :, i * width:(i + 1) * width] = val

    def expert_whole(n, first):
        s = lax.rem(first + n, DEPTH)
        u = n + AHEAD
        wait(expert_up(u, s))
        x = xbuf[rows_of(u), :]
        gate = jnp.dot(x, ring[s, 0], preferred_element_type=F32)
        up = jnp.dot(x, ring[s, 1], preferred_element_type=F32)
        act[rows_of(u), aligned(lax.rem(u, parts) * WIDTH, WIDTH)] = (jax.nn.silu(gate) * up).astype(BF16)
        issue(first + n + DEPTH)

        @pl.when(n == 0)
        def _():
            load_r.wait()
            logits = lax.dot_general(hbuf[me], wr[...], (((1,), (1,)), ((), ())), preferred_element_type=F32)
            prob[me] = jax.nn.softmax(logits, axis=-1)

        @pl.when(n == 1)
        def _():
            p_out[0].start()
            p_out[1].start()

        @pl.when(n == 4)
        def _():
            p_in[0].wait_recv()
            p_out[2].start()

        @pl.when(n == 6)
        def _():
            for copy in p_in[1:]:
                copy.wait_recv()
            for copy in p_out:
                copy.wait_send()

        @pl.when(lax.rem(n, n_full // group) == n_full // group - 2)
        def _():
            gates(n // (n_full // group))

    @pl.loop(0, BETWEEN)
    def _(n):
        expert_whole(n, first_m)

    @pl.loop(0, AHEAD)
    def _(u):
        s = lax.rem(first_b + u, DEPTH)
        wait(expert_up(u, s, k_early, hidden))
        x = xbuf[rows_of(u), k_early:hidden]
        gate = jnp.dot(x, ring[s, 0, 0:hidden - k_early, :], preferred_element_type=F32)
        up = jnp.dot(x, ring[s, 1, 0:hidden - k_early, :], preferred_element_type=F32)
        for half in range(2):
            cols = slice(half * CHUNK, (half + 1) * CHUNK)
            g = work[4 * u + half, 0:rows, :] + gate[:, cols]
            v = work[4 * u + 2 + half, 0:rows, :] + up[:, cols]
            act[rows_of(u), aligned(lax.rem(u, parts) * WIDTH + half * CHUNK, CHUNK)] = (jax.nn.silu(g) * v).astype(BF16)
        issue(first_b + u + DEPTH)

    pl.semaphore_signal(credit, inc=2, device_id={'ep': sib}, device_id_type=MESH)
    pl.semaphore_signal(ready, inc=1, device_id={'ep': far}, device_id_type=MESH)
    for i in range(PIECES):
        send_h(i).wait_send()
        pass_h(i).wait_send()
    send_sib().wait_send()
    for copy in idx_out:
        copy.wait_send()

    @pl.loop(BETWEEN, n_full)
    def _(n):
        expert_whole(n, first_g - BETWEEN)

    def send_pair(j):
        at = 2 * n_chunk
        return remote(work.at[at + 4:at + 6], work.at[pl.ds(at + 2 * lax.rem(j, 2), 2)], pair_send, pair_recv.at[lax.rem(j, 2)], sib)

    def send_relay(j):
        return remote(work.at[j], work.at[n_chunk + j], relay_send.at[j], relay_recv.at[j], far)

    def hand_over(j):
        send_pair(j).wait()
        got = 2 * n_chunk + 2 * lax.rem(j, 2)
        cols = aligned(j * CHUNK, CHUNK)
        work[j] = work[j] + work[got + 1]
        acc[:, cols] = acc[:, cols] + work[got]

        @pl.when(j == 0)
        def _():
            pl.semaphore_wait(ready, 1)

        send_relay(j).start()

        @pl.when(j < n_chunk - 2)
        def _():
            pl.semaphore_signal(credit, inc=1, device_id={'ep': sib}, device_id_type=MESH)

    def combined(dst):
        mixed = xbuf[aligned(dst * width, width), 0:CHUNK]
        total = jnp.dot(hbuf[dst, :, 0:width], mixed, preferred_element_type=F32)
        for i in range(1, 3):
            total = total + jnp.dot(hbuf[dst, :, i * width:(i + 1) * width], mixed, preferred_element_type=F32)
        return total

    @pl.loop(0, n_d)
    def _(n):
        s = lax.rem(first_d + n, DEPTH)
        j, quad = n // quads, lax.rem(n, quads)
        wait(expert_down(n, s))
        for i in range(4):
            e = quad * 4 + i
            res = jnp.dot(act[aligned(e * rows, rows), :], down_part(s, i)[...], preferred_element_type=F32).astype(BF16)
            for dst in range(group):
                xbuf[aligned(dst * width + e * local_max, local_max), 0:CHUNK] = res[dst * local_max:(dst + 1) * local_max, :]
        issue(first_d + n + DEPTH)

        @pl.when(jnp.logical_and(quad == 0, j > 1))
        def _():
            hand_over(j - 1)

        @pl.when(quad == quads - 1)
        def _():
            work[2 * n_chunk + 4] = combined(sib)
            work[2 * n_chunk + 5] = combined(diag)
            pl.semaphore_wait(credit, 1)
            send_pair(j).start()
            work[j] = combined(far)
            cols = aligned(j * CHUNK, CHUNK)
            acc[:, cols] = acc[:, cols] + combined(me)

            @pl.when(j == 0)
            def _():
                hand_over(0)

    hand_over(n_chunk - 1)

    def put(j):
        cols = aligned(j * CHUNK, CHUNK)
        return pltpu.make_async_copy(xbuf.at[0:tok, cols], out_hbm.at[:, cols], out_sem.at[j])

    @pl.loop(0, n_chunk)
    def _(j):
        cols = aligned(j * CHUNK, CHUNK)
        send_relay(j).wait()
        xbuf[0:tok, cols] = (acc[:, cols] + work[n_chunk + j]).astype(BF16)
        put(j).start()

    @pl.loop(0, n_chunk)
    def _(j):
        put(j).wait()


def moe(hidden_in, idx_t, gain, w_router, wsg, s_gate, s_up, s_down, w_gate, w_up, w_down, group, capacity, local_max):
    tok, hidden = hidden_in.shape
    slots, _, ff = w_gate.shape
    experts = w_router.shape[0]
    rows = group * local_max
    chunks = hidden // CHUNK
    vmem, dma = pltpu.VMEM, pltpu.SemaphoreType.DMA
    hbm_spec, vmem_spec = pl.BlockSpec(memory_space=pl.ANY), pl.BlockSpec(memory_space=pltpu.VMEM)
    return pl.pallas_call(
        functools.partial(moe_kernel, group, experts, capacity, local_max),
        out_shape=jax.ShapeDtypeStruct((tok, hidden), BF16),
        in_specs=[hbm_spec, vmem_spec, vmem_spec, hbm_spec, vmem_spec] + [hbm_spec] * 6,
        out_specs=hbm_spec,
        scratch_shapes=[
            vmem((DEPTH, 2, hidden, WIDTH), BF16),
            vmem((slots * rows, hidden), BF16),
            vmem((slots * rows, ff), BF16),
            vmem((group, tok, hidden), BF16),
            vmem((max(2 * chunks + 6, 4 * AHEAD), tok, CHUNK), F32),
            vmem((tok, hidden), F32),
            vmem((group, tok, experts), F32),
            vmem((group, experts, tok), F32),
            vmem((tok, 128), F32),
            vmem((group,) + idx_t.shape, jnp.int32),
            vmem((experts, hidden), BF16),
            vmem((experts, 128), F32),
            dma((DEPTH, 4)), dma((2,)), dma((chunks,)),
            dma((3,)), dma((3,)), dma((PIECES,)), dma((PIECES,)), dma, dma, dma((PIECES,)), dma((PIECES,)),
            dma((3,)), dma((3,)), dma, dma((2,)), dma((chunks,)), dma((chunks,)), pltpu.SemaphoreType.REGULAR, pltpu.SemaphoreType.REGULAR,
        ],
        compiler_params=pltpu.CompilerParams(collective_id=0, has_side_effects=True, vmem_limit_bytes=67043328),
        cost_estimate=pl.CostEstimate(flops=6 * slots * rows * hidden * ff, bytes_accessed=6 * slots * hidden * ff, transcendentals=0),
        name="moe",
    )(hidden_in, idx_t, gain, w_router, wsg, s_gate, s_up, s_down, w_gate, w_up, w_down)


def solution(mesh):
    group = mesh.shape['ep']

    def device_block(hidden_in, topk_idx, norm_gain, w_router, w_sgate, s_gate, s_up, s_down, w_gate, w_up, w_down):
        tok_dev, hidden = hidden_in.shape
        top_k = topk_idx.shape[1]
        experts = w_router.shape[1]
        capacity = (5 * tok_dev * group * top_k + 4 * experts - 1) // (4 * experts)
        local_max = (2 * tok_dev * top_k + experts - 1) // experts
        return moe(hidden_in, topk_idx.T, norm_gain, w_router.T, w_sgate.reshape(1, hidden),
                   s_gate, s_up, s_down, w_gate, w_up, w_down, group, capacity, local_max)

    row_spec = P(('dp', 'ep'), None)
    full_spec = P(None, None)
    slot_spec = P('ep', None, None)
    in_specs = (row_spec, row_spec, P(None), full_spec, full_spec, full_spec, full_spec, full_spec,
                slot_spec, slot_spec, slot_spec)
    return jax.shard_map(device_block, mesh=mesh, in_specs=in_specs, out_specs=row_spec, check_vma=False)
```
